32 devices in a mesh: cls: 4 (over y, x), dom: 8 (over z, core).
Axes of the slice: x: 2, y: 2, z: 4, core: 2. Of those that a mesh axis runs over, the one named last changes fastest.
Arguments:
- particles: bfloat16 [256, 2, 110592], P(('cls', 'dom')), may hold values from -18 to 18
- labels: int32 [256, 1], P(('cls', 'dom')), may hold values from 0 to 7; in each aligned block of 8 rows (0 to 7, 8 to 15, ...) at most 2 rows name the same one
- wedge_index: int32 [256], P(('cls', 'dom')), may hold values from 0 to 11
- wedge_table: float32 [12, 110592], replicated, may hold values from 0.05 to 1
Outputs:
- class_average: float32 [8, 2, 110592], P('cls', None, 'dom')
- weight_total: float32 [8, 110592], P('cls', 'dom')
The draws below stay inside these ranges and needn't reach their ends.
Inputs may be any that keep to these rules, and one draw needn't show every extreme that they name: `labels`: among the rows of one device no class appears more than 2 times, and on some devices one class appears exactly 2 times; every class appears on some device.
All inputs are finite; a program needn't handle non-finite values.
Results may differ from the reference program's by a relative error of at most 0.0003.
Values may be sent and summed in bfloat16 or wider, within the bound.
No kernel may reach another device: no remote copies, remote signals or barrier semaphores. Data moves between devices by JAX's collectives and lax.ppermute only.
A program may use at most 128 MiB of HBM per device.

```python
import math
import jax
import jax.numpy as jnp
import numpy as np
from jax import lax

P_DEV = 8
WEDGES = 12
CLASSES = 8
MOST = 2
VOX = 110592
PARTICLES = 256


def place_ends(values, stream_key, least, top_value):
    dims = values.shape
    index_at = [jax.random.randint(jax.random.fold_in(stream_key, axis), (), 0, dims[axis]) for axis in range(len(dims))]
    values = values.at[tuple(index_at)].set(least)
    longest = dims.index(max(dims))
    index_at[longest] = (index_at[longest] + 1) % dims[longest]
    return values.at[tuple(index_at)].set(top_value)


def level_of(key, shape, pieces, least, high):
    level = 1.0
    for position, parts in pieces:
        draws = jax.random.uniform(jax.random.fold_in(jax.random.fold_in(key, 6), position), (parts,), jnp.float32, least / len(pieces), high / len(pieces))
        level = level * jnp.repeat(jnp.exp(draws), shape[position] // parts).reshape((-1,) + (1,) * (len(shape) - 1 - position))
    return level


def shared_out(own_key, own, number, rows, count, top, limit, slope):
    ranking = jax.random.permutation(own_key, count)
    heavy_load, ordinary = shares(count, rows * top, limit, slope, True), shares(count, rows * top, limit, slope, False)
    places = jnp.arange(count)

    def named(tallies, turn):
        used = int((tallies > 0).sum())
        fixed = max(1, used // 4)
        shifted = fixed + (places - fixed + turn * (used - fixed)) % max(1, count - fixed)
        return jnp.zeros((count,), jnp.int32).at[ranking[jnp.where(places < fixed, places, shifted)]].set(jnp.asarray(tallies, jnp.int32))

    tallies = jnp.where(number % 4 == 0, named(heavy_load, number // 4), named(ordinary, number - number // 4 - 1))
    mixed = jax.random.permutation(jax.random.fold_in(own, 3), count)
    donor, taker = mixed[0:count // 2 * 2:2], mixed[1:count // 2 * 2:2]
    slack = jnp.minimum(tallies[donor] - 1, limit - tallies[taker]) // 2
    slack = jnp.where((donor == ranking[0]) | (taker == ranking[0]) | (tallies[taker] == 0), 0, jnp.maximum(slack, 0))
    shifted = jax.random.randint(jax.random.fold_in(own, 4), (count // 2,), 0, 1 << 20) % (slack + 1)
    tallies = tallies.at[donor].add(-shifted).at[taker].add(shifted)
    items = jnp.searchsorted(jnp.cumsum(tallies), jnp.arange(rows * top), side="right").astype(jnp.int32)
    grid = items.reshape(top, rows).T
    grid = grid[jax.random.permutation(jax.random.fold_in(own, 1), rows)]
    turn = jax.random.randint(jax.random.fold_in(own, 2), (rows, 1), 0, top)
    return jnp.take_along_axis(grid, (jnp.arange(top)[None, :] + turn) % top, axis=1)


def shares(number_of, total, bound, skew, full):
    loads = [(1 << 20) // math.isqrt(standing ** skew) + 1 for standing in range(1, number_of + 1)]
    largest = bound if full else min(bound, max(-(-total // number_of), total * loads[0] // sum(loads)))
    least = 1 if total - largest >= number_of - 1 else 0
    holding, surplus = [largest] + [least] * (number_of - 1), total - largest - least * (number_of - 1)
    while surplus > 0:
        free = [i for i in range(1, number_of) if holding[i] < largest] or [i for i in range(1, number_of) if holding[i] < bound]
        mass, remaining = sum([loads[i] for i in free]), surplus
        for i in free:
            extra = min(bound - holding[i], max(1, remaining * loads[i] // mass), surplus)
            holding[i] = holding[i] + extra
            surplus = surplus - extra
    return np.array(holding)


def bell_draw(rng, shape, spread, limit, split=(), kind=jnp.bfloat16):
    array = spread * jax.random.normal(rng, shape, jnp.float32)
    if split:
        array = array * level_of(rng, shape, split, -0.22, 0.18)
    return jnp.clip(array, -limit, limit).astype(kind)


def setup_inputs(seed: int = 0) -> dict:
    keys = jax.random.split(jax.random.key(seed), 5)
    particles = bell_draw(keys[0], (PARTICLES, 2, VOX), 3.0, 18.0, ((0, 32),))
    labels_keys = jax.random.split(jax.random.fold_in(keys[1], 1), PARTICLES // P_DEV)
    labels_turns = jax.random.permutation(jax.random.fold_in(keys[1], 3), PARTICLES // P_DEV)
    labels = jax.vmap(lambda own, number: shared_out(jax.random.fold_in(keys[1], 2), own, number, P_DEV, CLASSES, 1, MOST, 2))(labels_keys, labels_turns).reshape((PARTICLES, 1))
    wedge_index = place_ends(jax.random.randint(keys[2], (PARTICLES,), 0, WEDGES), jax.random.fold_in(keys[2], 1), 0, WEDGES - 1).astype(jnp.int32)
    wedge_table = jnp.clip(jnp.exp(jax.random.uniform(keys[3], (WEDGES, VOX), jnp.float32, math.log(0.05), math.log(1.0))), 0.05, 1.0)
    return {"particles": particles, "labels": labels, "wedge_index": wedge_index, "wedge_table": wedge_table}


def reference(particles, labels, wedge_index, wedge_table):
    count = particles.shape[0]
    block = 64 if count % 64 == 0 else count
    steps_total = count // block
    classes_all = CLASSES
    label_flat = labels[:, 0]

    def accumulate(carry, index):
        start = (index * block).astype(jnp.int32)
        piece = lax.dynamic_slice_in_dim(particles, start, block, 0).astype(jnp.float32)
        label_piece = lax.dynamic_slice_in_dim(label_flat, start, block, 0)
        wedge_piece = lax.dynamic_slice_in_dim(wedge_index, start, block, 0)
        pick = (wedge_piece[:, None] == jnp.arange(WEDGES, dtype=jnp.int32)[None, :]).astype(jnp.float32)
        weight = jnp.dot(pick, wedge_table, precision=lax.Precision.HIGHEST)
        member = (jnp.arange(classes_all, dtype=jnp.int32)[:, None] == label_piece[None, :]).astype(jnp.float32)
        numer = jnp.einsum("kb,bcv->kcv", member, weight[:, None, :] * piece, precision=lax.Precision.HIGHEST)
        denom = jnp.dot(member, weight * weight, precision=lax.Precision.HIGHEST)
        return (carry[0] + numer, carry[1] + denom), None

    start_sums = (jnp.zeros((classes_all, 2, VOX), jnp.float32), jnp.zeros((classes_all, VOX), jnp.float32))
    (weighted_sum, weight_total), unused = lax.scan(accumulate, start_sums, jnp.arange(steps_total, dtype=jnp.int32))
    class_average = weighted_sum / (weight_total[:, None, :] + 1.0)
    return class_average, weight_total
```

```python
import functools

import jax
import jax.numpy as jnp
from jax import lax
from jax.experimental import pallas as pl
from jax.experimental.pallas import tpu as pltpu
from jax.sharding import PartitionSpec as P

LANES = 128
SUB = 8
CORES = 2
STEPS = 8
TOP = 32000.0
LEAST = 1e-30
VMEM = pl.BlockSpec(memory_space=pltpu.VMEM)
SMEM = pl.BlockSpec(memory_space=pltpu.SMEM)
PARAMS = pltpu.CompilerParams(vmem_limit_bytes=40 * 1024 * 1024)


def padded(rows):
    return -(-(rows + 2) // SUB) * SUB


def partner(index, offset, count):
    if count & (count - 1) == 0:
        return index ^ offset
    return lax.rem(index + offset, count)


def back(index, offset, count):
    if count & (count - 1) == 0:
        return index ^ offset
    return lax.rem(index + count - offset, count)


def pack(total, counts):
    rows = total.shape[0]
    peak = jnp.maximum(jnp.max(jnp.abs(total), axis=0, keepdims=True), LEAST)
    level = jnp.ceil(jnp.log2(peak) * STEPS)
    inverse = TOP * jnp.exp2(level * (-1.0 / STEPS))
    coded = jnp.round(total * inverse)
    extra = padded(rows) - rows
    place = lax.broadcasted_iota(jnp.int32, (extra, LANES), 0)
    tail = jnp.where(place == 0, level, jnp.where(place == 1, counts, 0.0))
    return jnp.concatenate([coded, tail], axis=0).astype(jnp.int32).astype(jnp.int16)


def unpack(coded, rows):
    wide = coded.astype(jnp.int32).astype(jnp.float32)
    scale = jnp.exp2(wide[rows : rows + 1] * (1.0 / STEPS)) * (1.0 / TOP)
    return wide[:rows] * scale, wide[rows + 1 : rows + 2]


def class_counts(metas, classes, lane_shape):
    lane = lax.broadcasted_iota(jnp.int32, lane_shape, 1)
    rows = [jnp.zeros(lane_shape, jnp.float32) for _ in range(classes)]
    for meta in metas:
        for p in range(meta.shape[1]):
            hit = lane == meta[1, p]
            for k in range(classes):
                rows[k] = rows[k] + jnp.where(hit & (meta[0, p] == k), 1.0, 0.0)
    return rows


def accumulate(metas, sources, tab, zz, total):
    total[...] = jnp.zeros_like(total)
    for meta, source in zip(metas, sources):

        def add(p, carry):
            k = meta[0, p]
            weight = tab[meta[1, p], zz]
            for c in range(CORES):
                total[k, c] += weight * source[p, c, zz].astype(jnp.float32)
            return carry

        lax.fori_loop(0, source.shape[0], add, 0)


def sum_first(n_cls, n_z, by_z, own_meta, got_meta, pos, own, got, tab, *rest):
    outs, total, count_rows = rest[:-2], rest[-2], rest[-1]
    metas, sources = (own_meta, got_meta), (own, got)
    classes = total.shape[0]
    held = classes // n_cls
    for k, row in enumerate(class_counts(metas, classes, (SUB, LANES))):
        count_rows[k] = row
    for j in range(n_z):
        zz = partner(pos[1], j, n_z)
        accumulate(metas, sources, tab, zz, total)
        if by_z:
            for k in range(classes):
                for c in range(2):
                    outs[j][k, c] = pack(total[k, c], count_rows[k, 0:1])
        else:
            for i in range(n_cls):
                to = partner(pos[0], i, n_cls)
                for h in range(held):
                    k = to * held + h
                    for c in range(2):
                        outs[c * n_cls + i][h, zz] = pack(total[k, c], count_rows[k, 0:1])


def join(parts, index, rows):
    value, counts = unpack(parts[0][index], rows)
    for part in parts[1:]:
        more, extra = unpack(part[index], rows)
        value, counts = value + more, counts + extra
    return value, counts


def sum_cls(n_cls, n_z, rows, pos, *refs):
    parts, outs = refs[:n_cls], refs[n_cls:]
    for j in range(n_z):
        zz = partner(pos[1], j, n_z)
        for h in range(parts[0].shape[0]):
            outs[j][h] = pack(*join(parts, (h, zz), rows))


def sum_z(n_cls, n_z, rows, pos, *refs):
    parts, outs = refs[:n_z], refs[n_z:]
    held = parts[0].shape[0] // n_cls
    for i in range(n_cls):
        to = partner(pos[0], i, n_cls)
        for h in range(held):
            for c in range(2):
                outs[i][h, c] = pack(*join(parts, (to * held + h, c), rows))


def finish(n_cls, n_z, rows_a, rows_b, pos, tab_a, tab_b, *refs):
    planes = [refs[c * n_z : (c + 1) * n_z] for c in range(2)]
    tail = refs[2 * n_z : 2 * n_z + n_cls]
    average, weights = refs[2 * n_z + n_cls :]
    lane = lax.broadcasted_iota(jnp.int32, (1, LANES), 1)
    for h in range(average.shape[0]):
        sums = [join(planes[c], (h,), rows_a) for c in range(2)]
        ends = [join(tail, (h, c), rows_b) for c in range(2)]
        counts = sums[0][1]
        weight_a = jnp.zeros((rows_a, LANES), jnp.float32)
        weight_b = jnp.zeros((rows_b, LANES), jnp.float32)
        for w in range(tab_a.shape[0]):
            number = jnp.sum(jnp.where(lane == w, counts, 0.0), axis=1, keepdims=True)
            weight_a = weight_a + number * (tab_a[w, pos[1]] * tab_a[w, pos[1]])
            weight_b = weight_b + number * (tab_b[w, pos[1]] * tab_b[w, pos[1]])
        weights[h, :rows_a] = weight_a
        weights[h, rows_a:] = weight_b
        for c in range(2):
            average[h, c, :rows_a] = sums[c][0] / (weight_a + 1.0)
            average[h, c, rows_a:] = ends[c][0] / (weight_b + 1.0)


def call(body, operands, shapes, scratch=(), smem=1, cost=1 << 20):
    return pl.pallas_call(
        body,
        out_shape=shapes,
        in_specs=[SMEM] * smem + [VMEM] * (len(operands) - smem),
        out_specs=[VMEM] * len(shapes),
        scratch_shapes=list(scratch),
        compiler_params=PARAMS,
        cost_estimate=pl.CostEstimate(flops=cost, bytes_accessed=cost, transcendentals=0),
    )(*operands)


def per_device(n_class, particles, labels, wedge_index, wedge_table):
    n_cls, n_dom = lax.axis_size("cls"), lax.axis_size("dom")
    n_z = n_dom // CORES
    p_dev, parts, voxels = particles.shape
    rows = voxels // (n_dom * LANES)
    held = n_class // n_cls
    dom = lax.axis_index("dom")
    core = lax.rem(dom, CORES)
    pos = jnp.stack([lax.axis_index("cls"), dom // CORES]).astype(jnp.int32)

    swap = [(d, d ^ 1) for d in range(n_dom)]
    z_moves = [
        [(d, int(partner_of(d // CORES, j, n_z)) * CORES + d % CORES) for d in range(n_dom)]
        for j in range(n_z)
    ]
    cls_moves = [[(d, int(partner_of(d, i, n_cls))) for d in range(n_cls)] for i in range(n_cls)]

    meta = jnp.stack([labels[:, 0], wedge_index])
    got_meta = lax.ppermute(meta, "dom", swap)

    rows_a = -(-(rows * 72 // 100) // SUB) * SUB - 2
    cuts = ((0, rows_a), (rows_a, rows))
    wide = particles.reshape(p_dev, parts, n_z, CORES, rows, LANES)
    table = wedge_table.reshape(-1, n_z, CORES, rows, LANES)
    own, got, tab = [], [], []
    for low, high in cuts:
        piece = wide[:, :, :, :, low:high]
        away = lax.dynamic_index_in_dim(piece, 1 - core, 3, keepdims=False)
        got.append(lax.ppermute(away, "dom", swap))
        own.append(lax.dynamic_index_in_dim(piece, core, 3, keepdims=False))
        tab.append(lax.dynamic_index_in_dim(table[:, :, :, low:high], core, 2, keepdims=False))

    rows_b = rows - rows_a
    size_a, size_b = padded(rows_a), padded(rows_b)

    def ints(*dims):
        return jax.ShapeDtypeStruct(dims + (LANES,), jnp.int16)

    def first(which, by_z, shapes):
        return call(
            functools.partial(sum_first, n_cls, n_z, by_z),
            (meta, got_meta, pos, own[which], got[which], tab[which]),
            shapes,
            scratch=(
                pltpu.VMEM((n_class, parts) + own[which].shape[-2:], jnp.float32),
                pltpu.VMEM((n_class, SUB, LANES), jnp.float32),
            ),
            smem=3,
        )

    head = first(0, False, [ints(held, n_z, size_a)] * (parts * n_cls))
    ends = first(1, True, [ints(n_class, parts, size_b)] * n_z)

    def over(axis, moves, arrays):
        return [arrays[0]] + [lax.ppermute(a, axis, m) for a, m in zip(arrays[1:], moves[1:])]

    moved = [over("cls", cls_moves, head[c * n_cls : (c + 1) * n_cls]) for c in range(parts)]
    ends = over("dom", z_moves, ends)
    planes = []
    for c in range(parts):
        coded = call(
            functools.partial(sum_cls, n_cls, n_z, rows_a),
            (pos, *moved[c]),
            [ints(held, size_a)] * n_z,
        )
        planes.extend(over("dom", z_moves, coded))
    coded = call(
        functools.partial(sum_z, n_cls, n_z, rows_b),
        (pos, *ends),
        [ints(held, parts, size_b)] * n_cls,
    )
    ends = over("cls", cls_moves, coded)
    average, weights = call(
        functools.partial(finish, n_cls, n_z, rows_a, rows_b),
        (pos, tab[0], tab[1], *planes, *ends),
        [
            jax.ShapeDtypeStruct((held, parts, rows, LANES), jnp.float32),
            jax.ShapeDtypeStruct((held, rows, LANES), jnp.float32),
        ],
    )
    return average.reshape(held, parts, -1), weights.reshape(held, -1)


def partner_of(index, offset, count):
    return index ^ offset if count & (count - 1) == 0 else (index + offset) % count


def solution(mesh):
    n_class = 2 * mesh.shape["cls"]
    return jax.shard_map(
        functools.partial(per_device, n_class),
        mesh=mesh,
        in_specs=(P(("cls", "dom"), None, None), P(("cls", "dom"), None), P(("cls", "dom")), P()),
        out_specs=(P("cls", None, "dom"), P("cls", "dom")),
        check_vma=False,
    )
```

```python
import functools

import jax
import jax.numpy as jnp
from jax import lax
from jax.experimental import pallas as pl
from jax.experimental.layout import Layout, with_layout_constraint
from jax.experimental.pallas import tpu as pltpu
from jax.sharding import PartitionSpec as P


CLS_GROUP = 2
LANES = 128
SUB = 8
CORES = 2
PARTS = 2
STEPS = 8
TOP = 32000.0
LEAST = 1e-30
VMEM = pl.BlockSpec(memory_space=pltpu.VMEM)
SMEM = pl.BlockSpec(memory_space=pltpu.SMEM)
ANY = pl.BlockSpec(memory_space=pl.ANY)
DMA = pltpu.SemaphoreType.DMA


def up(rows, step=SUB):
    return -(-rows // step) * step


def coded_rows(rows):
    return up(rows) + SUB


def partner(index, offset, count):
    if count & (count - 1) == 0:
        return index ^ offset
    return (index + offset) % count


def pack(total, counts):
    rows = total.shape[0]
    peak = jnp.maximum(jnp.max(jnp.abs(total), axis=0, keepdims=True), LEAST)
    level = jnp.ceil(jnp.log2(peak) * STEPS)
    inverse = TOP * jnp.exp2(level * (-1.0 / STEPS))
    coded = jnp.round(total * inverse)
    extra = coded_rows(rows) - rows
    place = lax.broadcasted_iota(jnp.int32, (extra, LANES), 0)
    tail = jnp.where(place == 0, level, jnp.where(place == 1, counts, 0.0))
    return jnp.concatenate([coded, tail], axis=0).astype(jnp.int32).astype(jnp.int16)


def unpack(coded, rows):
    wide = coded.astype(jnp.int32).astype(jnp.float32)
    scale = jnp.exp2(wide[rows : rows + 1] * (1.0 / STEPS)) * (1.0 / TOP)
    return wide[:rows] * scale, wide[rows + 1 : rows + 2]


def join(parts, index, rows):
    value, counts = unpack(parts[0][index], rows)
    for part in parts[1:]:
        more, extra = unpack(part[index], rows)
        value, counts = value + more, counts + extra
    return value, counts


def split(cuts, pos, wide, *rest):
    outs, sems = rest[: len(cuts)], rest[-1]
    n_z = outs[0].shape[1]
    copies = []
    for i, (low, high) in enumerate(cuts):
        for z in range(n_z):
            source = wide.at[:, z * CORES + 1 - pos[2], low:high]
            copies.append(pltpu.make_async_copy(source, outs[i].at[:, z], sems.at[i, z]))
    for copy in copies:
        copy.start()
    for copy in copies:
        copy.wait()


def own_sums(pos, meta, table, wide, weights, total, table_buf, wide_buf, sems):
    n_z, p_dev, rows = wide_buf.shape[:3]
    wedges, length = table_buf.shape[1:]
    stride = weights.shape[1] // wedges
    copies = []
    for z in range(n_z):
        shard = z * CORES + pos[2]
        source = table.at[:, pl.ds(pl.multiple_of(shard * length, LANES), length)]
        first = pltpu.make_async_copy(source, table_buf.at[z], sems.at[0, z])
        second = pltpu.make_async_copy(wide.at[:, shard], wide_buf.at[z], sems.at[1, z])
        first.start()
        second.start()
        copies.append((first, second))
    for z in range(n_z):
        copies[z][0].wait()
        for t in range(rows // PARTS):
            for base in range(0, wedges, SUB):
                count = min(SUB, wedges - base)
                tile = table_buf[z, base : base + count, t * LANES : (t + 1) * LANES]
                for c in range(PARTS):
                    weights[z, pl.ds(base * stride + t * PARTS + c, count, stride=stride), :] = tile
        copies[z][1].wait()
        for k in range(total.shape[0]):
            total[k, z] = jnp.zeros_like(total[k, z])

        def add(p, carry):
            start = pl.multiple_of(meta[1, p] * stride, SUB)
            total[meta[0, p], z] += weights[z, pl.ds(start, rows), :] * wide_buf[z, p].astype(jnp.float32)
            return carry

        lax.fori_loop(0, p_dev, add, 0)


def chip_sums(n_cls, n_z, by_z, low, stride, pos, own_meta, got_meta, got, weights, begun, *rest):
    outs, total, tally = rest[:-2], rest[-2], rest[-1]
    classes, rows = total.shape[0], total.shape[1]
    held = classes // n_cls
    lane = lax.broadcasted_iota(jnp.int32, (SUB, LANES), 1)
    for k in range(classes):
        tally[k] = jnp.zeros((SUB, LANES), jnp.float32)
    for meta in (own_meta, got_meta):

        def mark(p, carry):
            tally[meta[0, p]] += jnp.where(lane == meta[1, p], 1.0, 0.0)
            return carry

        lax.fori_loop(0, meta.shape[1], mark, 0)
    for j in range(n_z):
        zz = partner(pos[1], j, n_z)
        for k in range(classes):
            total[k] = begun[k, zz, low : low + rows]

        def add(p, carry):
            start = pl.multiple_of(got_meta[1, p] * stride + low, SUB)
            total[got_meta[0, p]] += weights[zz, pl.ds(start, rows), :] * got[p, zz].astype(jnp.float32)
            return carry

        lax.fori_loop(0, got.shape[0], add, 0)
        if by_z:
            for k in range(classes):
                outs[j][k] = pack(total[k], tally[k, 0:1])
        else:
            for i in range(n_cls):
                to = partner(pos[0], i, n_cls)
                for h in range(held):
                    k = to * held + h
                    outs[i][h, zz] = pack(total[k], tally[k, 0:1])


def sum_cls(n_cls, n_z, rows, pos, *refs):
    parts, outs = refs[:n_cls], refs[n_cls:]
    for j in range(n_z):
        zz = partner(pos[1], j, n_z)
        for h in range(parts[0].shape[0]):
            outs[j][h] = pack(*join(parts, (h, zz), rows))


def sum_z(n_cls, n_z, rows, pos, *refs):
    parts, outs = refs[:n_z], refs[n_z:]
    held = parts[0].shape[0] // n_cls
    for i in range(n_cls):
        to = partner(pos[0], i, n_cls)
        for h in range(held):
            outs[i][h] = pack(*join(parts, (to * held + h,), rows))


def finish(n_cls, n_z, cuts, wedges, pos, weights, *refs):
    sides = (refs[:n_z], refs[n_z : n_z + n_cls])
    average, totals, scratch = refs[n_z + n_cls :]
    stride = weights.shape[1] // wedges
    held, rows = average.shape[0], average.shape[1]
    lane = lax.broadcasted_iota(jnp.int32, (1, LANES), 1)
    for h in range(held):
        counts = None
        for parts, (low, high) in zip(sides, cuts):
            sums, found = join(parts, (h,), high - low)
            counts = found if counts is None else counts
            weight = jnp.zeros((high - low, LANES), jnp.float32)
            for w in range(wedges):
                number = jnp.sum(jnp.where(lane == w, counts, 0.0), axis=1, keepdims=True)
                one = weights[pos[1], w * stride + low : w * stride + high]
                weight = weight + number * (one * one)
            scratch[low:high] = weight
            average[h, low:high] = sums / (weight + 1.0)
        totals[pl.ds(h, rows // PARTS, stride=held), :] = scratch[pl.ds(0, rows // PARTS, stride=PARTS), :]


def call(body, operands, specs, shapes, scratch=(), flops=1 << 22, limit=48):
    return pl.pallas_call(
        body,
        out_shape=shapes,
        in_specs=specs,
        out_specs=[VMEM] * len(shapes),
        scratch_shapes=list(scratch),
        compiler_params=pltpu.CompilerParams(vmem_limit_bytes=limit * 1024 * 1024),
        cost_estimate=pl.CostEstimate(flops=flops, bytes_accessed=flops, transcendentals=0),
    )(*operands)


def per_device(particles, labels, wedge_index, wedge_table):
    n_cls, n_dom = lax.axis_size("cls"), lax.axis_size("dom")
    n_z = n_dom // CORES
    n_class = n_cls * CLS_GROUP
    p_dev, parts, voxels = particles.shape
    wedges = wedge_table.shape[0]
    tiles = voxels // (n_dom * LANES)
    rows = tiles * parts
    stride = up(rows)
    dom = lax.axis_index("dom")
    pos = jnp.stack([lax.axis_index("cls"), dom // CORES, dom % CORES]).astype(jnp.int32)

    swap = [(d, d ^ 1) for d in range(n_dom)]
    z_moves = [
        [(d, partner(d // CORES, j, n_z) * CORES + d % CORES) for d in range(n_dom)] for j in range(n_z)
    ]
    cls_moves = [[(d, partner(d, i, n_cls)) for d in range(n_cls)] for i in range(n_cls)]

    cut = rows * 71 // 100 // SUB * SUB
    cuts = ((0, cut), (cut, rows))
    wide = particles.reshape(p_dev, parts, n_dom * tiles, LANES).transpose(0, 2, 1, 3)
    wide = wide.reshape(p_dev, n_dom, rows, LANES)

    def array(dims, kind):
        return jax.ShapeDtypeStruct(dims + (LANES,), kind)

    meta = jnp.stack([labels[:, 0], wedge_index])
    away = call(
        functools.partial(split, cuts),
        (pos, wide),
        [SMEM, ANY],
        [array((p_dev, n_z, high - low), wide.dtype) for low, high in cuts],
        scratch=[DMA((len(cuts), n_z))],
    )
    got_meta = lax.ppermute(meta, "dom", swap)
    got = [lax.ppermute(a, "dom", swap) for a in away]
    weights, begun = call(
        own_sums,
        (pos, meta, wedge_table, wide),
        [SMEM, SMEM, ANY, ANY],
        [array((n_z, wedges * stride), jnp.float32), array((n_class, n_z, rows), jnp.float32)],
        scratch=[
            pltpu.VMEM((n_z, wedges, tiles * LANES), jnp.float32),
            pltpu.VMEM((n_z, p_dev, rows, LANES), wide.dtype),
            DMA((2, n_z)),
        ],
        flops=1 << 24,
    )

    def chip(which, by_z, shapes):
        low, high = cuts[which]
        return call(
            functools.partial(chip_sums, n_cls, n_z, by_z, low, stride),
            (pos, meta, got_meta, got[which], weights, begun),
            [SMEM] * 3 + [VMEM] * 3,
            shapes,
            scratch=[
                pltpu.VMEM((n_class, high - low, LANES), jnp.float32),
                pltpu.VMEM((n_class, SUB, LANES), jnp.float32),
            ],
        )

    def over(axis, moves, arrays):
        return [arrays[0]] + [lax.ppermute(a, axis, m) for a, m in zip(arrays[1:], moves[1:])]

    def fold(body, count, which, arrays, shapes):
        low, high = cuts[which]
        return call(
            functools.partial(body, n_cls, n_z, high - low),
            (pos, *arrays),
            [SMEM] + [VMEM] * count,
            shapes,
        )

    size = [coded_rows(high - low) for low, high in cuts]
    head = over("cls", cls_moves, chip(0, False, [array((CLS_GROUP, n_z, size[0]), jnp.int16)] * n_cls))
    ends = over("dom", z_moves, chip(1, True, [array((n_class, size[1]), jnp.int16)] * n_z))
    head = fold(sum_cls, n_cls, 0, head, [array((CLS_GROUP, size[0]), jnp.int16)] * n_z)
    head = over("dom", z_moves, head)
    ends = fold(sum_z, n_z, 1, ends, [array((CLS_GROUP, size[1]), jnp.int16)] * n_cls)
    ends = over("cls", cls_moves, ends)
    average, totals = call(
        functools.partial(finish, n_cls, n_z, cuts, wedges),
        (pos, weights, *head, *ends),
        [SMEM] + [VMEM] * (1 + n_z + n_cls),
        [array((CLS_GROUP, rows), jnp.float32), array((tiles * CLS_GROUP,), jnp.float32)],
        scratch=[pltpu.VMEM((rows, LANES), jnp.float32)],
    )
    average = average.reshape(CLS_GROUP, tiles, parts, LANES).transpose(0, 2, 1, 3)
    average = with_layout_constraint(average, Layout(major_to_minor=(0, 2, 1, 3)))
    totals = totals.reshape(tiles, CLS_GROUP, LANES).transpose(1, 0, 2)
    totals = with_layout_constraint(totals, Layout(major_to_minor=(1, 0, 2)))
    return average.reshape(CLS_GROUP, parts, -1), totals.reshape(CLS_GROUP, -1)


def solution(mesh):
    return jax.shard_map(
        per_device,
        mesh=mesh,
        in_specs=(P(("cls", "dom"), None, None), P(("cls", "dom"), None), P(("cls", "dom")), P()),
        out_specs=(P("cls", None, "dom"), P("cls", "dom")),
        check_vma=False,
    )
```

```python
import functools

import jax
import jax.numpy as jnp
from jax import lax
from jax.experimental import pallas as pl
from jax.experimental.layout import Layout, with_layout_constraint
from jax.experimental.pallas import tpu as pltpu
from jax.sharding import PartitionSpec as P


CLS_GROUP = 2
LANES = 128
SUB = 8
CORES = 2
PARTS = 2
STEPS = 8
TOP = 32000.0
LEAST = 1e-30
VMEM = pl.BlockSpec(memory_space=pltpu.VMEM)
SMEM = pl.BlockSpec(memory_space=pltpu.SMEM)
HBM = pl.BlockSpec(memory_space=pltpu.HBM)
DMA = pltpu.SemaphoreType.DMA


def up(rows, step=SUB):
    return -(-rows // step) * step


def coded_rows(rows):
    return up(rows) + SUB


def partner(index, offset, count):
    return (index + offset) % count


def pack(total, counts):
    rows = total.shape[0]
    peak = jnp.maximum(jnp.max(jnp.abs(total), axis=0, keepdims=True), LEAST)
    level = jnp.ceil(jnp.log2(peak) * STEPS)
    inverse = TOP * jnp.exp2(level * (-1.0 / STEPS))
    coded = jnp.round(total * inverse)
    extra = coded_rows(rows) - rows
    place = lax.broadcasted_iota(jnp.int32, (extra, LANES), 0)
    tail = jnp.where(place == 0, level, jnp.where(place == 1, counts, 0.0))
    return jnp.concatenate([coded, tail], axis=0).astype(jnp.int32).astype(jnp.int16)


def unpack(coded, rows):
    wide = coded.astype(jnp.int32).astype(jnp.float32)
    scale = jnp.exp2(wide[rows : rows + 1] * (1.0 / STEPS)) * (1.0 / TOP)
    return wide[:rows] * scale, wide[rows + 1 : rows + 2]


def join(parts, index, rows):
    value, counts = unpack(parts[0][index], rows)
    for part in parts[1:]:
        more, extra = unpack(part[index], rows)
        value, counts = value + more, counts + extra
    return value, counts


def split(cuts, pos, wide, *rest):
    outs, sems = rest[: len(cuts)], rest[-1]
    n_z = outs[0].shape[1]
    copies = []
    for i, (low, high) in enumerate(cuts):
        for z in range(n_z):
            source = wide.at[:, z * CORES + 1 - pos[2], low:high]
            copies.append(pltpu.make_async_copy(source, outs[i].at[:, z], sems.at[i, z]))
    for copy in copies:
        copy.start()
    for copy in copies:
        copy.wait()


def own_sums(pos, meta, table, wide, weights, total, table_buf, wide_buf, sems):
    n_z, p_dev, rows = wide_buf.shape[:3]
    wedges, length = table_buf.shape[1:]
    stride = weights.shape[1] // wedges
    copies = []
    for z in range(n_z):
        shard = z * CORES + pos[2]
        source = table.at[:, pl.ds(pl.multiple_of(shard * length, LANES), length)]
        first = pltpu.make_async_copy(source, table_buf.at[z], sems.at[0, z])
        second = pltpu.make_async_copy(wide.at[:, shard], wide_buf.at[z], sems.at[1, z])
        first.start()
        second.start()
        copies.append((first, second))
    for z in range(n_z):
        copies[z][0].wait()
        for t in range(rows // PARTS):
            for base in range(0, wedges, SUB):
                count = min(SUB, wedges - base)
                tile = table_buf[z, base : base + count, t * LANES : (t + 1) * LANES]
                for c in range(PARTS):
                    weights[z, pl.ds(base * stride + t * PARTS + c, count, stride=stride), :] = tile
        copies[z][1].wait()
        for k in range(total.shape[0]):
            total[k, z] = jnp.zeros_like(total[k, z])

        def add(p, carry):
            start = pl.multiple_of(meta[1, p] * stride, SUB)
            total[meta[0, p], z] += weights[z, pl.ds(start, rows), :] * wide_buf[z, p].astype(jnp.float32)
            return carry

        lax.fori_loop(0, p_dev, add, 0)


def chip_sums(n_cls, n_z, by_z, low, stride, pos, own_meta, got_meta, got, weights, begun, *rest):
    outs, total, tally = rest[:-2], rest[-2], rest[-1]
    classes, rows = total.shape[0], total.shape[1]
    held = classes // n_cls
    lane = lax.broadcasted_iota(jnp.int32, (SUB, LANES), 1)
    for k in range(classes):
        tally[k] = jnp.zeros((SUB, LANES), jnp.float32)
    for meta in (own_meta, got_meta):

        def mark(p, carry):
            tally[meta[0, p]] += jnp.where(lane == meta[1, p], 1.0, 0.0)
            return carry

        lax.fori_loop(0, meta.shape[1], mark, 0)
    for j in range(n_z):
        zz = partner(pos[1], j, n_z)
        for k in range(classes):
            total[k] = begun[k, zz, low : low + rows]

        def add(p, carry):
            start = pl.multiple_of(got_meta[1, p] * stride + low, SUB)
            total[got_meta[0, p]] += weights[zz, pl.ds(start, rows), :] * got[p, zz].astype(jnp.float32)
            return carry

        lax.fori_loop(0, got.shape[0], add, 0)
        if by_z:
            for k in range(classes):
                outs[j][k] = pack(total[k], tally[k, 0:1])
        else:
            for i in range(n_cls):
                to = partner(pos[0], i, n_cls)
                for h in range(held):
                    k = to * held + h
                    outs[i][h, zz] = pack(total[k], tally[k, 0:1])


def sum_cls(n_cls, n_z, rows, pos, *refs):
    parts, outs = refs[:n_cls], refs[n_cls:]
    for j in range(n_z):
        zz = partner(pos[1], j, n_z)
        for h in range(parts[0].shape[0]):
            outs[j][h] = pack(*join(parts, (h, zz), rows))


def sum_z(n_cls, n_z, rows, pos, *refs):
    parts, outs = refs[:n_z], refs[n_z:]
    held = parts[0].shape[0] // n_cls
    for i in range(n_cls):
        to = partner(pos[0], i, n_cls)
        for h in range(held):
            outs[i][h] = pack(*join(parts, (to * held + h,), rows))


def finish(n_cls, n_z, cuts, wedges, pos, weights, *refs):
    sides = (refs[:n_z], refs[n_z : n_z + n_cls])
    average, totals, scratch = refs[n_z + n_cls :]
    stride = weights.shape[1] // wedges
    held, rows = average.shape[0], average.shape[1]
    lane = lax.broadcasted_iota(jnp.int32, (1, LANES), 1)
    for h in range(held):
        counts = None
        for parts, (low, high) in zip(sides, cuts):
            sums, found = join(parts, (h,), high - low)
            counts = found if counts is None else counts
            weight = jnp.zeros((high - low, LANES), jnp.float32)
            for w in range(wedges):
                number = jnp.sum(jnp.where(lane == w, counts, 0.0), axis=1, keepdims=True)
                one = weights[pos[1], w * stride + low : w * stride + high]
                weight = weight + number * (one * one)
            scratch[low:high] = weight
            average[h, low:high] = sums / (weight + 1.0)
        totals[pl.ds(h, rows // PARTS, stride=held), :] = scratch[pl.ds(0, rows // PARTS, stride=PARTS), :]


def call(body, operands, specs, shapes, scratch=(), flops=1 << 22, limit=16):
    return pl.pallas_call(
        body,
        out_shape=shapes,
        in_specs=specs,
        out_specs=[VMEM] * len(shapes),
        scratch_shapes=list(scratch),
        compiler_params=pltpu.CompilerParams(vmem_limit_bytes=limit * 1024 * 1024),
        cost_estimate=pl.CostEstimate(flops=flops, bytes_accessed=flops, transcendentals=0),
    )(*operands)


def per_device(particles, labels, wedge_index, wedge_table):
    n_cls, n_dom = lax.axis_size("cls"), lax.axis_size("dom")
    n_z = n_dom // CORES
    n_class = n_cls * CLS_GROUP
    p_dev, parts, voxels = particles.shape
    wedges = wedge_table.shape[0]
    tiles = voxels // (n_dom * LANES)
    rows = tiles * parts
    stride = up(rows)
    dom = lax.axis_index("dom")
    pos = jnp.stack([lax.axis_index("cls"), dom // CORES, dom % CORES]).astype(jnp.int32)

    swap = [(d, d ^ 1) for d in range(n_dom)]
    z_moves = [
        [(d, partner(d // CORES, j, n_z) * CORES + d % CORES) for d in range(n_dom)] for j in range(n_z)
    ]
    cls_moves = [[(d, partner(d, i, n_cls)) for d in range(n_cls)] for i in range(n_cls)]

    cut = rows * 71 // 100 // SUB * SUB
    cuts = ((0, cut), (cut, rows))
    wide = particles.reshape(p_dev, parts, n_dom * tiles, LANES).transpose(0, 2, 1, 3)
    wide = wide.reshape(p_dev, n_dom, rows, LANES)

    def array(dims, kind):
        return jax.ShapeDtypeStruct(dims + (LANES,), kind)

    def held_in_hbm(value):
        return pltpu.with_memory_space_constraint(value, pltpu.HBM)

    meta = jnp.stack([labels[:, 0], wedge_index])
    away = call(
        functools.partial(split, cuts),
        (pos, held_in_hbm(wide)),
        [SMEM, HBM],
        [array((p_dev, n_z, high - low), wide.dtype) for low, high in cuts],
        scratch=[DMA((len(cuts), n_z))],
    )
    got_meta = lax.ppermute(meta, "dom", swap)
    got = [lax.ppermute(a, "dom", swap) for a in away]
    weights, begun = call(
        own_sums,
        (pos, meta, held_in_hbm(wedge_table), held_in_hbm(wide)),
        [SMEM, SMEM, HBM, HBM],
        [array((n_z, wedges * stride), jnp.float32), array((n_class, n_z, rows), jnp.float32)],
        scratch=[
            pltpu.VMEM((n_z, wedges, tiles * LANES), jnp.float32),
            pltpu.VMEM((n_z, p_dev, rows, LANES), wide.dtype),
            DMA((2, n_z)),
        ],
        flops=1 << 24,
    )

    def chip(which, by_z, shapes):
        low, high = cuts[which]
        return call(
            functools.partial(chip_sums, n_cls, n_z, by_z, low, stride),
            (pos, meta, got_meta, got[which], weights, begun),
            [SMEM] * 3 + [VMEM] * 3,
            shapes,
            scratch=[
                pltpu.VMEM((n_class, high - low, LANES), jnp.float32),
                pltpu.VMEM((n_class, SUB, LANES), jnp.float32),
            ],
        )

    def over(axis, moves, arrays):
        return [arrays[0]] + [lax.ppermute(a, axis, m) for a, m in zip(arrays[1:], moves[1:])]

    def fold(body, count, which, arrays, shapes):
        low, high = cuts[which]
        return call(
            functools.partial(body, n_cls, n_z, high - low),
            (pos, *arrays),
            [SMEM] + [VMEM] * count,
            shapes,
        )

    size = [coded_rows(high - low) for low, high in cuts]
    head = over("cls", cls_moves, chip(0, False, [array((CLS_GROUP, n_z, size[0]), jnp.int16)] * n_cls))
    ends = over("dom", z_moves, chip(1, True, [array((n_class, size[1]), jnp.int16)] * n_z))
    head = fold(sum_cls, n_cls, 0, head, [array((CLS_GROUP, size[0]), jnp.int16)] * n_z)
    head = over("dom", z_moves, head)
    ends = fold(sum_z, n_z, 1, ends, [array((CLS_GROUP, size[1]), jnp.int16)] * n_cls)
    ends = over("cls", cls_moves, ends)
    average, totals = call(
        functools.partial(finish, n_cls, n_z, cuts, wedges),
        (pos, weights, *head, *ends),
        [SMEM] + [VMEM] * (1 + n_z + n_cls),
        [array((CLS_GROUP, rows), jnp.float32), array((tiles * CLS_GROUP,), jnp.float32)],
        scratch=[pltpu.VMEM((rows, LANES), jnp.float32)],
    )
    average = average.reshape(CLS_GROUP, tiles, parts, LANES).transpose(0, 2, 1, 3)
    average = with_layout_constraint(average, Layout(major_to_minor=(0, 2, 1, 3)))
    totals = totals.reshape(tiles, CLS_GROUP, LANES).transpose(1, 0, 2)
    totals = with_layout_constraint(totals, Layout(major_to_minor=(1, 0, 2)))
    return average.reshape(CLS_GROUP, parts, -1), totals.reshape(CLS_GROUP, -1)


def solution(mesh):
    return jax.shard_map(
        per_device,
        mesh=mesh,
        in_specs=(P(("cls", "dom"), None, None), P(("cls", "dom"), None), P(("cls", "dom")), P()),
        out_specs=(P("cls", None, "dom"), P("cls", "dom")),
        check_vma=False,
    )
```

```python
import functools

import jax
import jax.numpy as jnp
from jax import lax
from jax.experimental import pallas as pl
from jax.experimental.layout import Layout, with_layout_constraint
from jax.experimental.pallas import tpu as pltpu
from jax.sharding import PartitionSpec as P


CLS_GROUP = 2
LANES = 128
SUB = 8
CORES = 2
PARTS = 2
STEPS = 8
CUT = 67
TOP = 32000.0
LEAST = 1e-30
VMEM = pl.BlockSpec(memory_space=pltpu.VMEM)
SMEM = pl.BlockSpec(memory_space=pltpu.SMEM)
HBM = pl.BlockSpec(memory_space=pltpu.HBM)
DMA = pltpu.SemaphoreType.DMA


def up(rows, step=SUB):
    return -(-rows // step) * step


def partner(index, offset, count):
    if count & (count - 1) == 0:
        return index ^ offset
    return (index + offset) % count


def tiles_of(first, rows):
    return (up(rows) - SUB, SUB - 2) if first else (0, 0)


def pack(total, counts, first):
    rows = total.shape[0]
    base, place = tiles_of(first, rows)
    row = lax.broadcasted_iota(jnp.int32, (SUB, LANES), 0)
    edge = total[base : base + SUB]
    edge = jnp.where(row < SUB - 2 if first else row >= SUB - 2, edge, 0.0)
    pieces = [total[:base], edge] if first else [edge, total[SUB:]]
    peak = jnp.full((1, LANES), LEAST, jnp.float32)
    for piece in pieces:
        peak = jnp.maximum(peak, jnp.max(jnp.abs(piece), axis=0, keepdims=True))
    level = jnp.ceil(jnp.log2(peak) * STEPS)
    inverse = TOP * jnp.exp2(level * (-1.0 / STEPS))
    coded = [jnp.round(piece * inverse) for piece in pieces]
    at = 1 if first else 0
    coded[at] = jnp.where(row == place, level, jnp.where(row == place + 1, counts, coded[at]))
    return jnp.concatenate(coded, axis=0).astype(jnp.int32).astype(jnp.int16)


def unpack(coded, first):
    base, place = tiles_of(first, coded.shape[0])
    wide = coded.astype(jnp.int32).astype(jnp.float32)
    at = base + place
    scale = jnp.exp2(wide[at : at + 1] * (1.0 / STEPS)) * (1.0 / TOP)
    return wide * scale, wide[at + 1 : at + 2]


def join(parts, index, first):
    value, counts = unpack(parts[0][index], first)
    for part in parts[1:]:
        more, extra = unpack(part[index], first)
        value, counts = value + more, counts + extra
    return value, counts


def split(cuts, pos, wide, *rest):
    outs, sems = rest[: len(cuts)], rest[-1]
    n_z = outs[0].shape[1]
    copies = []
    for i, (low, high) in enumerate(cuts):
        for z in range(n_z):
            source = wide.at[:, z * CORES + 1 - pos[2], low:high]
            copies.append(pltpu.make_async_copy(source, outs[i].at[:, z], sems.at[i, z]))
    for copy in copies:
        copy.start()
    for copy in copies:
        copy.wait()


def own_sums(pos, meta, table, wide, weights, total, table_buf, wide_buf, sems):
    n_z, p_dev, rows = wide_buf.shape[:3]
    wedges, length = table_buf.shape[1:]
    stride = weights.shape[1] // wedges
    copies = []
    for z in range(n_z):
        shard = z * CORES + pos[2]
        source = table.at[:, pl.ds(pl.multiple_of(shard * length, LANES), length)]
        first = pltpu.make_async_copy(source, table_buf.at[z], sems.at[0, z])
        second = pltpu.make_async_copy(wide.at[:, shard], wide_buf.at[z], sems.at[1, z])
        first.start()
        second.start()
        copies.append((first, second))
    for z in range(n_z):
        for k in range(total.shape[0]):
            total[k, z] = jnp.zeros_like(total[k, z])
    for z in range(n_z):
        copies[z][0].wait()
        for t in range(rows // PARTS):
            for base in range(0, wedges, SUB):
                count = min(SUB, wedges - base)
                tile = table_buf[z, base : base + count, t * LANES : (t + 1) * LANES]
                for c in range(PARTS):
                    weights[z, pl.ds(base * stride + t * PARTS + c, count, stride=stride), :] = tile
        copies[z][1].wait()

        def add(p, carry):
            start = pl.multiple_of(meta[1, p] * stride, SUB)
            total[meta[0, p], z] += weights[z, pl.ds(start, rows), :] * wide_buf[z, p].astype(jnp.float32)
            return carry

        lax.fori_loop(0, p_dev, add, 0)


def chip_sums(n_cls, n_z, by_z, low, stride, pos, own_meta, got_meta, got, weights, begun, *rest):
    outs, total, tally = rest[:-2], rest[-2], rest[-1]
    classes, rows = total.shape[0], total.shape[1]
    held = classes // n_cls
    lane = lax.broadcasted_iota(jnp.int32, (SUB, LANES), 1)
    for k in range(classes):
        tally[k] = jnp.zeros((SUB, LANES), jnp.float32)
    for meta in (own_meta, got_meta):

        def mark(p, carry):
            tally[meta[0, p]] += jnp.where(lane == meta[1, p], 1.0, 0.0)
            return carry

        lax.fori_loop(0, meta.shape[1], mark, 0)
    for j in range(n_z):
        zz = partner(pos[1], j, n_z)
        for k in range(classes):
            total[k] = begun[k, zz, low : low + rows]

        def add(p, carry):
            start = pl.multiple_of(got_meta[1, p] * stride + low, SUB)
            total[got_meta[0, p]] += weights[zz, pl.ds(start, rows), :] * got[p, zz].astype(jnp.float32)
            return carry

        lax.fori_loop(0, got.shape[0], add, 0)
        if by_z:
            for k in range(classes):
                outs[j][k] = pack(total[k], tally[k, 0:1], False)
        else:
            for i in range(n_cls):
                to = partner(pos[0], i, n_cls)
                for h in range(held):
                    k = to * held + h
                    outs[i][h, zz] = pack(total[k], tally[k, 0:1], True)


def sum_cls(n_cls, n_z, pos, *refs):
    parts, outs = refs[:n_cls], refs[n_cls:]
    for j in range(n_z):
        zz = partner(pos[1], j, n_z)
        for h in range(parts[0].shape[0]):
            outs[j][h] = pack(*join(parts, (h, zz), True), True)


def sum_z(n_cls, n_z, pos, *refs):
    parts, outs = refs[:n_z], refs[n_z:]
    held = parts[0].shape[0] // n_cls
    for i in range(n_cls):
        to = partner(pos[0], i, n_cls)
        for h in range(held):
            outs[i][h] = pack(*join(parts, (to * held + h,), False), False)


def finish(n_cls, n_z, cuts, wedges, pos, weights, *refs):
    sides = (refs[:n_z], refs[n_z : n_z + n_cls])
    average, totals, scratch = refs[n_z + n_cls :]
    stride = weights.shape[1] // wedges
    held, rows = average.shape[0], average.shape[1]
    shape = (up(wedges), LANES)
    lane, place = lax.broadcasted_iota(jnp.int32, shape, 1), lax.broadcasted_iota(jnp.int32, shape, 0)
    heads = [join(sides[0], (h,), True) for h in range(held)]
    ends = [join(sides[1], (h,), False)[0] for h in range(held)]
    numbers = [
        jnp.sum(jnp.where(lane == place, counts, 0.0), axis=1, keepdims=True) for _, counts in heads
    ]
    cut = cuts[1][0]
    row = lax.broadcasted_iota(jnp.int32, (SUB, LANES), 0)
    pieces = ((0, cut), (cut, cut + SUB), (cut + SUB, rows))
    for low, high in pieces:
        weight = [jnp.zeros((high - low, LANES), jnp.float32) for _ in range(held)]
        for w in range(wedges):
            one = weights[pos[1], w * stride + low : w * stride + high]
            square = one * one
            for h in range(held):
                weight[h] = weight[h] + numbers[h][w : w + 1] * square
        for h in range(held):
            if low == 0:
                sums = heads[h][0][:cut]
            elif low == cut:
                sums = jnp.where(row < SUB - 2, heads[h][0][cut:], ends[h][:SUB])
            else:
                sums = ends[h][SUB:]
            scratch[h, low:high] = weight[h]
            average[h, low:high] = sums / (weight[h] + 1.0)
    for h in range(held):
        tiles = rows // PARTS
        totals[pl.ds(h, tiles, stride=held), :] = scratch[h, pl.ds(0, tiles, stride=PARTS), :]


def call(body, operands, specs, shapes, scratch=(), flops=1 << 22, limit=16):
    return pl.pallas_call(
        body,
        out_shape=shapes,
        in_specs=specs,
        out_specs=[VMEM] * len(shapes),
        scratch_shapes=list(scratch),
        compiler_params=pltpu.CompilerParams(vmem_limit_bytes=limit * 1024 * 1024),
        cost_estimate=pl.CostEstimate(flops=flops, bytes_accessed=flops, transcendentals=0),
    )(*operands)


def per_device(particles, labels, wedge_index, wedge_table):
    n_cls, n_dom = lax.axis_size("cls"), lax.axis_size("dom")
    n_z = n_dom // CORES
    n_class = n_cls * CLS_GROUP
    p_dev, parts, voxels = particles.shape
    wedges = wedge_table.shape[0]
    tiles = voxels // (n_dom * LANES)
    rows = tiles * parts
    stride = up(rows)
    dom = lax.axis_index("dom")
    pos = jnp.stack([lax.axis_index("cls"), dom // CORES, dom % CORES]).astype(jnp.int32)

    swap = [(d, d ^ 1) for d in range(n_dom)]
    z_moves = [
        [(d, partner(d // CORES, j, n_z) * CORES + d % CORES) for d in range(n_dom)] for j in range(n_z)
    ]
    cls_moves = [[(d, partner(d, i, n_cls)) for d in range(n_cls)] for i in range(n_cls)]

    cut = rows * CUT // 100 // SUB * SUB
    cuts = ((0, cut + SUB), (cut, rows))
    wide = particles.reshape(p_dev, parts, n_dom * tiles, LANES).transpose(0, 2, 1, 3)
    wide = wide.reshape(p_dev, n_dom, rows, LANES)

    def array(dims, kind):
        return jax.ShapeDtypeStruct(dims + (LANES,), kind)

    def held_in_hbm(value):
        return pltpu.with_memory_space_constraint(value, pltpu.HBM)

    meta = jnp.stack([labels[:, 0], wedge_index])
    away = call(
        functools.partial(split, cuts),
        (pos, held_in_hbm(wide)),
        [SMEM, HBM],
        [array((p_dev, n_z, high - low), wide.dtype) for low, high in cuts],
        scratch=[DMA((len(cuts), n_z))],
    )
    got_meta = lax.ppermute(meta, "dom", swap)
    got = [lax.ppermute(a, "dom", swap) for a in away]
    weights, begun = call(
        own_sums,
        (pos, meta, held_in_hbm(wedge_table), held_in_hbm(wide)),
        [SMEM, SMEM, HBM, HBM],
        [array((n_z, wedges * stride), jnp.float32), array((n_class, n_z, rows), jnp.float32)],
        scratch=[
            pltpu.VMEM((n_z, wedges, tiles * LANES), jnp.float32),
            pltpu.VMEM((n_z, p_dev, rows, LANES), wide.dtype),
            DMA((2, n_z)),
        ],
        flops=1 << 24,
    )

    def chip(which, by_z, shapes):
        low, high = cuts[which]
        return call(
            functools.partial(chip_sums, n_cls, n_z, by_z, low, stride),
            (pos, meta, got_meta, got[which], weights, begun),
            [SMEM] * 3 + [VMEM] * 3,
            shapes,
            scratch=[
                pltpu.VMEM((n_class, high - low, LANES), jnp.float32),
                pltpu.VMEM((n_class, SUB, LANES), jnp.float32),
            ],
        )

    def over(axis, moves, arrays):
        moved = list(arrays)
        for i in range(1, len(moves)):
            moved[i] = lax.ppermute(arrays[i], axis, moves[i])
        return moved

    def fold(body, count, arrays, shapes):
        return call(
            functools.partial(body, n_cls, n_z),
            (pos, *arrays),
            [SMEM] + [VMEM] * count,
            shapes,
        )

    size = [high - low for low, high in cuts]
    head = over("cls", cls_moves, chip(0, False, [array((CLS_GROUP, n_z, size[0]), jnp.int16)] * n_cls))
    ends = over("dom", z_moves, chip(1, True, [array((n_class, size[1]), jnp.int16)] * n_z))
    head = fold(sum_cls, n_cls, head, [array((CLS_GROUP, size[0]), jnp.int16)] * n_z)
    head = over("dom", z_moves, head)
    ends = fold(sum_z, n_z, ends, [array((CLS_GROUP, size[1]), jnp.int16)] * n_cls)
    ends = over("cls", cls_moves, ends)
    average, totals = call(
        functools.partial(finish, n_cls, n_z, cuts, wedges),
        (pos, weights, *head, *ends),
        [SMEM] + [VMEM] * (1 + n_z + n_cls),
        [array((CLS_GROUP, rows), jnp.float32), array((tiles * CLS_GROUP,), jnp.float32)],
        scratch=[pltpu.VMEM((CLS_GROUP, rows, LANES), jnp.float32)],
    )
    average = average.reshape(CLS_GROUP, tiles, parts, LANES).transpose(0, 2, 1, 3)
    average = with_layout_constraint(average, Layout(major_to_minor=(0, 2, 1, 3)))
    totals = totals.reshape(tiles, CLS_GROUP, LANES).transpose(1, 0, 2)
    totals = with_layout_constraint(totals, Layout(major_to_minor=(1, 0, 2)))
    return average.reshape(CLS_GROUP, parts, -1), totals.reshape(CLS_GROUP, -1)


def solution(mesh):
    return jax.shard_map(
        per_device,
        mesh=mesh,
        in_specs=(P(("cls", "dom"), None, None), P(("cls", "dom"), None), P(("cls", "dom")), P()),
        out_specs=(P("cls", None, "dom"), P("cls", "dom")),
        check_vma=False,
    )
```

```python
import functools

import jax
import jax.numpy as jnp
from jax import lax
from jax.experimental import pallas as pl
from jax.experimental.layout import Layout, with_layout_constraint
from jax.experimental.pallas import tpu as pltpu
from jax.sharding import PartitionSpec as P


CLS_GROUP = 2
LANES = 128
SUB = 8
CORES = 2
PARTS = 2
STEPS = 8
CUT = 67
TOP = 32000.0
LEAST = 1e-30
VMEM = pl.BlockSpec(memory_space=pltpu.VMEM)
HBM = pl.BlockSpec(memory_space=pltpu.HBM)
DMA = pltpu.SemaphoreType.DMA


def up(rows, step=SUB):
    return -(-rows // step) * step


def position():
    dom = lax.axis_index("dom")
    return lax.axis_index("cls"), lax.div(dom, CORES), lax.rem(dom, CORES)


def numbers_of(meta):
    found = meta[...]
    return [(found[0, p], found[1, p]) for p in range(meta.shape[1])]


def partner(index, offset, count):
    if count & (count - 1) == 0:
        return index ^ offset
    return (index + offset) % count


def tiles_of(first, rows):
    return (up(rows) - SUB, SUB - 2) if first else (0, 0)


def pack(total, counts, first):
    rows = total.shape[0]
    base, place = tiles_of(first, rows)
    row = lax.broadcasted_iota(jnp.int32, (SUB, LANES), 0)
    edge = total[base : base + SUB]
    edge = jnp.where(row < SUB - 2 if first else row >= SUB - 2, edge, 0.0)
    pieces = [total[:base], edge] if first else [edge, total[SUB:]]
    peak = jnp.full((1, LANES), LEAST, jnp.float32)
    for piece in pieces:
        peak = jnp.maximum(peak, jnp.max(jnp.abs(piece), axis=0, keepdims=True))
    level = jnp.ceil(jnp.log2(peak) * STEPS)
    inverse = TOP * jnp.exp2(level * (-1.0 / STEPS))
    coded = [jnp.round(piece * inverse) for piece in pieces]
    at = 1 if first else 0
    coded[at] = jnp.where(row == place, level, jnp.where(row == place + 1, counts, coded[at]))
    return jnp.concatenate(coded, axis=0).astype(jnp.int32).astype(jnp.int16)


def unpack(coded, first):
    base, place = tiles_of(first, coded.shape[0])
    wide = coded.astype(jnp.int32).astype(jnp.float32)
    at = base + place
    scale = jnp.exp2(wide[at : at + 1] * (1.0 / STEPS)) * (1.0 / TOP)
    return wide * scale, wide[at + 1 : at + 2]


def join(parts, index, first):
    value, counts = unpack(parts[0][index], first)
    for part in parts[1:]:
        more, extra = unpack(part[index], first)
        value, counts = value + more, counts + extra
    return value, counts


def split(cuts, wide, *rest):
    pos = position()
    outs, sems = rest[: len(cuts)], rest[-1]
    n_z = outs[0].shape[1]
    copies = []
    for i, (low, high) in enumerate(cuts):
        for z in range(n_z):
            source = wide.at[:, z * CORES + 1 - pos[2], low:high]
            copies.append(pltpu.make_async_copy(source, outs[i].at[:, z], sems.at[i, z]))
    for copy in copies:
        copy.start()
    for copy in copies:
        copy.wait()


def own_sums(meta, table, wide, weights, total, tally, table_buf, wide_buf, sems):
    pos = position()
    n_z, _, rows = wide_buf.shape[:3]
    wedges, length = table_buf.shape[1:]
    stride = weights.shape[1] // wedges
    copies = []
    for z in range(n_z):
        shard = z * CORES + pos[2]
        source = table.at[:, pl.ds(pl.multiple_of(shard * length, LANES), length)]
        first = pltpu.make_async_copy(source, table_buf.at[z], sems.at[0, z])
        second = pltpu.make_async_copy(wide.at[:, shard], wide_buf.at[z], sems.at[1, z])
        first.start()
        second.start()
        copies.append((first, second))
    named = numbers_of(meta)
    for z in range(n_z):
        for k in range(total.shape[0]):
            total[k, z] = jnp.zeros_like(total[k, z])
    tally[...] = jnp.zeros_like(tally)
    lane = lax.broadcasted_iota(jnp.int32, (SUB, LANES), 1)
    for k, w in named:
        tally[k] += jnp.where(lane == w, 1.0, 0.0)
    for z in range(n_z):
        copies[z][0].wait()
        for t in range(rows // PARTS):
            for base in range(0, wedges, SUB):
                count = min(SUB, wedges - base)
                tile = table_buf[z, base : base + count, t * LANES : (t + 1) * LANES]
                for c in range(PARTS):
                    weights[z, pl.ds(base * stride + t * PARTS + c, count, stride=stride), :] = tile
        copies[z][1].wait()

        for p, (k, w) in enumerate(named):
            start = pl.multiple_of(w * stride, SUB)
            total[k, z] += weights[z, pl.ds(start, rows), :] * wide_buf[z, p].astype(jnp.float32)


def chip_sums(n_cls, n_z, by_z, low, stride, got_meta, got, weights, begun, own_tally, *rest):
    pos = position()
    outs, total, tally = rest[:-2], rest[-2], rest[-1]
    classes, rows = total.shape[0], total.shape[1]
    held = classes // n_cls
    named = numbers_of(got_meta)
    lane = lax.broadcasted_iota(jnp.int32, (SUB, LANES), 1)
    tally[...] = own_tally[...]
    for k, w in named:
        tally[k] += jnp.where(lane == w, 1.0, 0.0)
    for j in range(n_z):
        zz = partner(pos[1], j, n_z)
        for k in range(classes):
            total[k] = begun[k, zz, low : low + rows]
        for p, (k, w) in enumerate(named):
            start = pl.multiple_of(w * stride + low, SUB)
            total[k] += weights[zz, pl.ds(start, rows), :] * got[p, zz].astype(jnp.float32)
        if by_z:
            for k in range(classes):
                outs[j][k] = pack(total[k], tally[k, 0:1], False)
        else:
            for i in range(n_cls):
                to = partner(pos[0], i, n_cls)
                for h in range(held):
                    k = to * held + h
                    outs[i][h, zz] = pack(total[k], tally[k, 0:1], True)


def sum_cls(n_cls, n_z, *refs):
    pos = position()
    parts, outs = refs[:n_cls], refs[n_cls:]
    for j in range(n_z):
        zz = partner(pos[1], j, n_z)
        for h in range(parts[0].shape[0]):
            outs[j][h] = pack(*join(parts, (h, zz), True), True)


def sum_z(n_cls, n_z, *refs):
    pos = position()
    parts, outs = refs[:n_z], refs[n_z:]
    held = parts[0].shape[0] // n_cls
    for i in range(n_cls):
        to = partner(pos[0], i, n_cls)
        for h in range(held):
            outs[i][h] = pack(*join(parts, (to * held + h,), False), False)


def finish(n_cls, n_z, cuts, wedges, weights, *refs):
    pos = position()
    sides = (refs[:n_z], refs[n_z : n_z + n_cls])
    average, totals, scratch = refs[n_z + n_cls :]
    stride = weights.shape[1] // wedges
    held, rows = average.shape[0], average.shape[1]
    shape = (up(wedges), LANES)
    lane, place = lax.broadcasted_iota(jnp.int32, shape, 1), lax.broadcasted_iota(jnp.int32, shape, 0)
    heads = [join(sides[0], (h,), True) for h in range(held)]
    ends = [join(sides[1], (h,), False)[0] for h in range(held)]
    numbers = [
        jnp.sum(jnp.where(lane == place, counts, 0.0), axis=1, keepdims=True) for _, counts in heads
    ]
    cut = cuts[1][0]
    row = lax.broadcasted_iota(jnp.int32, (SUB, LANES), 0)
    pieces = ((0, cut), (cut, cut + SUB), (cut + SUB, rows))
    for low, high in pieces:
        weight = [jnp.zeros((high - low, LANES), jnp.float32) for _ in range(held)]
        for w in range(wedges):
            one = weights[pos[1], w * stride + low : w * stride + high]
            square = one * one
            for h in range(held):
                weight[h] = weight[h] + numbers[h][w : w + 1] * square
        for h in range(held):
            if low == 0:
                sums = heads[h][0][:cut]
            elif low == cut:
                sums = jnp.where(row < SUB - 2, heads[h][0][cut:], ends[h][:SUB])
            else:
                sums = ends[h][SUB:]
            scratch[h, low:high] = weight[h]
            average[h, low:high] = sums / (weight[h] + 1.0)
    for h in range(held):
        tiles = rows // PARTS
        totals[pl.ds(h, tiles, stride=held), :] = scratch[h, pl.ds(0, tiles, stride=PARTS), :]


def call(body, operands, specs, shapes, scratch=(), flops=1 << 22, limit=16):
    return pl.pallas_call(
        body,
        out_shape=shapes,
        in_specs=specs,
        out_specs=[VMEM] * len(shapes),
        scratch_shapes=list(scratch),
        compiler_params=pltpu.CompilerParams(vmem_limit_bytes=limit * 1024 * 1024),
        cost_estimate=pl.CostEstimate(flops=flops, bytes_accessed=flops, transcendentals=0),
    )(*operands)


def per_device(particles, labels, wedge_index, wedge_table):
    n_cls, n_dom = lax.axis_size("cls"), lax.axis_size("dom")
    n_z = n_dom // CORES
    n_class = n_cls * CLS_GROUP
    p_dev, parts, voxels = particles.shape
    wedges = wedge_table.shape[0]
    tiles = voxels // (n_dom * LANES)
    rows = tiles * parts
    stride = up(rows)

    swap = [(d, d ^ 1) for d in range(n_dom)]
    z_moves = [
        [(d, partner(d // CORES, j, n_z) * CORES + d % CORES) for d in range(n_dom)] for j in range(n_z)
    ]
    cls_moves = [[(d, partner(d, i, n_cls)) for d in range(n_cls)] for i in range(n_cls)]

    cut = rows * CUT // 100 // SUB * SUB
    cuts = ((0, cut + SUB), (cut, rows))
    wide = particles.reshape(p_dev, parts, n_dom * tiles, LANES).transpose(0, 2, 1, 3)
    wide = wide.reshape(p_dev, n_dom, rows, LANES)

    def array(dims, kind):
        return jax.ShapeDtypeStruct(dims + (LANES,), kind)

    def held_in_hbm(value):
        return pltpu.with_memory_space_constraint(value, pltpu.HBM)

    meta = jnp.stack([labels[:, 0], wedge_index])
    away = call(
        functools.partial(split, cuts),
        (held_in_hbm(wide),),
        [HBM],
        [array((p_dev, n_z, high - low), wide.dtype) for low, high in cuts],
        scratch=[DMA((len(cuts), n_z))],
    )
    got_meta = lax.ppermute(meta, "dom", swap)
    got = [lax.ppermute(a, "dom", swap) for a in away]
    weights, begun, tally = call(
        own_sums,
        (meta, held_in_hbm(wedge_table), held_in_hbm(wide)),
        [VMEM, HBM, HBM],
        [array((n_z, wedges * stride), jnp.float32), array((n_class, n_z, rows), jnp.float32), array((n_class, SUB), jnp.float32)],
        scratch=[
            pltpu.VMEM((n_z, wedges, tiles * LANES), jnp.float32),
            pltpu.VMEM((n_z, p_dev, rows, LANES), wide.dtype),
            DMA((2, n_z)),
        ],
        flops=1 << 24,
    )

    def chip(which, by_z, shapes):
        low, high = cuts[which]
        return call(
            functools.partial(chip_sums, n_cls, n_z, by_z, low, stride),
            (got_meta, got[which], weights, begun, tally),
            [VMEM] * 5,
            shapes,
            scratch=[
                pltpu.VMEM((n_class, high - low, LANES), jnp.float32),
                pltpu.VMEM((n_class, SUB, LANES), jnp.float32),
            ],
        )

    def over(axis, moves, arrays):
        moved = list(arrays)
        for i in range(1, len(moves)):
            moved[i] = lax.ppermute(arrays[i], axis, moves[i])
        return moved

    def fold(body, count, arrays, shapes):
        return call(
            functools.partial(body, n_cls, n_z),
            tuple(arrays),
            [VMEM] * count,
            shapes,
        )

    size = [high - low for low, high in cuts]
    head = over("cls", cls_moves, chip(0, False, [array((CLS_GROUP, n_z, size[0]), jnp.int16)] * n_cls))
    ends = over("dom", z_moves, chip(1, True, [array((n_class, size[1]), jnp.int16)] * n_z))
    head = fold(sum_cls, n_cls, head, [array((CLS_GROUP, size[0]), jnp.int16)] * n_z)
    head = over("dom", z_moves, head)
    ends = fold(sum_z, n_z, ends, [array((CLS_GROUP, size[1]), jnp.int16)] * n_cls)
    ends = over("cls", cls_moves, ends)
    average, totals = call(
        functools.partial(finish, n_cls, n_z, cuts, wedges),
        (weights, *head, *ends),
        [VMEM] * (1 + n_z + n_cls),
        [array((CLS_GROUP, rows), jnp.float32), array((tiles * CLS_GROUP,), jnp.float32)],
        scratch=[pltpu.VMEM((CLS_GROUP, rows, LANES), jnp.float32)],
    )
    average = average.reshape(CLS_GROUP, tiles, parts, LANES).transpose(0, 2, 1, 3)
    average = with_layout_constraint(average, Layout(major_to_minor=(0, 2, 1, 3)))
    totals = totals.reshape(tiles, CLS_GROUP, LANES).transpose(1, 0, 2)
    totals = with_layout_constraint(totals, Layout(major_to_minor=(1, 0, 2)))
    return average.reshape(CLS_GROUP, parts, -1), totals.reshape(CLS_GROUP, -1)


def solution(mesh):
    return jax.shard_map(
        per_device,
        mesh=mesh,
        in_specs=(P(("cls", "dom"), None, None), P(("cls", "dom"), None), P(("cls", "dom")), P()),
        out_specs=(P("cls", None, "dom"), P("cls", "dom")),
        check_vma=False,
    )
```

```python
import functools

import jax
import jax.numpy as jnp
from jax import lax
from jax.experimental import pallas as pl
from jax.experimental.layout import Layout, with_layout_constraint
from jax.experimental.pallas import tpu as pltpu
from jax.sharding import PartitionSpec as P


CLS_GROUP = 2
LANES = 128
SUB = 8
CORES = 2
PARTS = 2
STEPS = 8
CUT = 63
TOP = 32000.0
LEAST = 1e-30
VMEM = pl.BlockSpec(memory_space=pltpu.VMEM)
HBM = pl.BlockSpec(memory_space=pltpu.HBM)
DMA = pltpu.SemaphoreType.DMA


def up(rows, step=SUB):
    return -(-rows // step) * step


def position():
    dom = lax.axis_index("dom")
    return lax.axis_index("cls"), lax.div(dom, CORES), lax.rem(dom, CORES)


def numbers_of(meta):
    found = meta[...]
    return [(found[0, p], found[1, p]) for p in range(meta.shape[1])]


def partner(index, offset, count):
    if count & (count - 1) == 0:
        return index ^ offset
    return (index + offset) % count


def tiles_of(first, rows):
    return (up(rows) - SUB, SUB - 2) if first else (0, 0)


def pack(total, counts, first):
    rows = total.shape[0]
    base, place = tiles_of(first, rows)
    row = lax.broadcasted_iota(jnp.int32, (SUB, LANES), 0)
    edge = total[base : base + SUB]
    edge = jnp.where(row < SUB - 2 if first else row >= SUB - 2, edge, 0.0)
    pieces = [total[:base], edge] if first else [edge, total[SUB:]]
    peak = jnp.full((1, LANES), LEAST, jnp.float32)
    for piece in pieces:
        peak = jnp.maximum(peak, jnp.max(jnp.abs(piece), axis=0, keepdims=True))
    level = jnp.ceil(jnp.log2(peak) * STEPS)
    inverse = TOP * jnp.exp2(level * (-1.0 / STEPS))
    coded = [jnp.round(piece * inverse) for piece in pieces]
    at = 1 if first else 0
    coded[at] = jnp.where(row == place, level, jnp.where(row == place + 1, counts, coded[at]))
    return jnp.concatenate(coded, axis=0).astype(jnp.int32).astype(jnp.int16)


def unpack(coded, first):
    base, place = tiles_of(first, coded.shape[0])
    wide = coded.astype(jnp.int32).astype(jnp.float32)
    at = base + place
    scale = jnp.exp2(wide[at : at + 1] * (1.0 / STEPS)) * (1.0 / TOP)
    return wide * scale, wide[at + 1 : at + 2]


def join(parts, index, first):
    value, counts = unpack(parts[0][index], first)
    for part in parts[1:]:
        more, extra = unpack(part[index], first)
        value, counts = value + more, counts + extra
    return value, counts


def split(cuts, wide, *rest):
    pos = position()
    outs, sems = rest[: len(cuts)], rest[-1]
    n_z = outs[0].shape[1]
    copies = []
    for i, (low, high) in enumerate(cuts):
        for z in range(n_z):
            source = wide.at[:, z * CORES + 1 - pos[2], low:high]
            copies.append(pltpu.make_async_copy(source, outs[i].at[:, z], sems.at[i, z]))
    for copy in copies:
        copy.start()
    for copy in copies:
        copy.wait()


def own_sums(meta, table, wide, weights, total, tally, table_buf, wide_buf, sems):
    pos = position()
    n_z, _, rows = wide_buf.shape[:3]
    wedges, length = table_buf.shape[1:]
    stride = weights.shape[1] // wedges
    copies = []
    for z in range(n_z):
        shard = z * CORES + pos[2]
        source = table.at[:, pl.ds(pl.multiple_of(shard * length, LANES), length)]
        first = pltpu.make_async_copy(source, table_buf.at[z], sems.at[0, z])
        second = pltpu.make_async_copy(wide.at[:, shard], wide_buf.at[z], sems.at[1, z])
        first.start()
        second.start()
        copies.append((first, second))
    named = numbers_of(meta)
    for z in range(n_z):
        for k in range(total.shape[0]):
            total[k, z] = jnp.zeros_like(total[k, z])
    tally[...] = jnp.zeros_like(tally)
    lane = lax.broadcasted_iota(jnp.int32, (SUB, LANES), 1)
    for k, w in named:
        tally[k] += jnp.where(lane == w, 1.0, 0.0)
    for z in range(n_z):
        copies[z][0].wait()
        for t in range(rows // PARTS):
            for base in range(0, wedges, SUB):
                count = min(SUB, wedges - base)
                tile = table_buf[z, base : base + count, t * LANES : (t + 1) * LANES]
                for c in range(PARTS):
                    weights[z, pl.ds(base * stride + t * PARTS + c, count, stride=stride), :] = tile
        copies[z][1].wait()

        for p, (k, w) in enumerate(named):
            start = pl.multiple_of(w * stride, SUB)
            total[k, z] += weights[z, pl.ds(start, rows), :] * wide_buf[z, p].astype(jnp.float32)


def chip_sums(n_cls, n_z, by_z, low, stride, got_meta, got, weights, begun, own_tally, *rest):
    pos = position()
    outs, total, tally = rest[:-2], rest[-2], rest[-1]
    classes, rows = total.shape[0], total.shape[1]
    held = classes // n_cls
    named = numbers_of(got_meta)
    lane = lax.broadcasted_iota(jnp.int32, (SUB, LANES), 1)
    tally[...] = own_tally[...]
    for k, w in named:
        tally[k] += jnp.where(lane == w, 1.0, 0.0)
    for j in range(n_z):
        zz = partner(pos[1], j, n_z)
        for k in range(classes):
            total[k] = begun[k, zz, low : low + rows]
        for p, (k, w) in enumerate(named):
            start = pl.multiple_of(w * stride + low, SUB)
            total[k] += weights[zz, pl.ds(start, rows), :] * got[p, zz].astype(jnp.float32)
        if by_z:
            for k in range(classes):
                outs[j][k] = pack(total[k], tally[k, 0:1], False)
        else:
            for i in range(n_cls):
                to = partner(pos[0], i, n_cls)
                for h in range(held):
                    k = to * held + h
                    outs[i][h, zz] = pack(total[k], tally[k, 0:1], True)


def sum_cls(n_cls, n_z, *refs):
    pos = position()
    parts, outs = refs[:n_cls], refs[n_cls:]
    for j in range(n_z):
        zz = partner(pos[1], j, n_z)
        for h in range(parts[0].shape[0]):
            outs[j][h] = pack(*join(parts, (h, zz), True), True)


def sum_z(n_cls, n_z, *refs):
    pos = position()
    parts, outs = refs[:n_z], refs[n_z:]
    held = parts[0].shape[0] // n_cls
    for i in range(n_cls):
        to = partner(pos[0], i, n_cls)
        for h in range(held):
            outs[i][h] = pack(*join(parts, (to * held + h,), False), False)


def finish(n_cls, n_z, cuts, wedges, weights, *refs):
    pos = position()
    sides = (refs[:n_z], refs[n_z : n_z + n_cls])
    average, totals, scratch = refs[n_z + n_cls :]
    stride = weights.shape[1] // wedges
    held, rows = average.shape[0], average.shape[1]
    shape = (up(wedges), LANES)
    lane, place = lax.broadcasted_iota(jnp.int32, shape, 1), lax.broadcasted_iota(jnp.int32, shape, 0)
    heads = [join(sides[0], (h,), True) for h in range(held)]
    ends = [join(sides[1], (h,), False)[0] for h in range(held)]
    numbers = [
        jnp.sum(jnp.where(lane == place, counts, 0.0), axis=1, keepdims=True) for _, counts in heads
    ]
    cut = cuts[1][0]
    row = lax.broadcasted_iota(jnp.int32, (SUB, LANES), 0)
    pieces = ((0, cut), (cut, cut + SUB), (cut + SUB, rows))
    for low, high in pieces:
        weight = [jnp.zeros((high - low, LANES), jnp.float32) for _ in range(held)]
        for w in range(wedges):
            one = weights[pos[1], w * stride + low : w * stride + high]
            square = one * one
            for h in range(held):
                weight[h] = weight[h] + numbers[h][w : w + 1] * square
        for h in range(held):
            if low == 0:
                sums = heads[h][0][:cut]
            elif low == cut:
                sums = jnp.where(row < SUB - 2, heads[h][0][cut:], ends[h][:SUB])
            else:
                sums = ends[h][SUB:]
            scratch[h, low:high] = weight[h]
            average[h, low:high] = sums / (weight[h] + 1.0)
    for h in range(held):
        tiles = rows // PARTS
        totals[pl.ds(h, tiles, stride=held), :] = scratch[h, pl.ds(0, tiles, stride=PARTS), :]


def call(body, operands, specs, shapes, scratch=(), flops=1 << 22, limit=16):
    return pl.pallas_call(
        body,
        out_shape=shapes,
        in_specs=specs,
        out_specs=[VMEM] * len(shapes),
        scratch_shapes=list(scratch),
        compiler_params=pltpu.CompilerParams(vmem_limit_bytes=limit * 1024 * 1024),
        cost_estimate=pl.CostEstimate(flops=flops, bytes_accessed=flops, transcendentals=0),
    )(*operands)


def per_device(particles, labels, wedge_index, wedge_table):
    n_cls, n_dom = lax.axis_size("cls"), lax.axis_size("dom")
    n_z = n_dom // CORES
    n_class = n_cls * CLS_GROUP
    p_dev, parts, voxels = particles.shape
    wedges = wedge_table.shape[0]
    tiles = voxels // (n_dom * LANES)
    rows = tiles * parts
    stride = up(rows)

    swap = [(d, d ^ 1) for d in range(n_dom)]
    z_moves = [
        [(d, partner(d // CORES, j, n_z) * CORES + d % CORES) for d in range(n_dom)] for j in range(n_z)
    ]
    cls_moves = [[(d, partner(d, i, n_cls)) for d in range(n_cls)] for i in range(n_cls)]

    cut = rows * CUT // 100 // SUB * SUB
    cuts = ((0, cut + SUB), (cut, rows))
    wide = particles.reshape(p_dev, parts, n_dom * tiles, LANES).transpose(0, 2, 1, 3)
    wide = wide.reshape(p_dev, n_dom, rows, LANES)

    def array(dims, kind):
        return jax.ShapeDtypeStruct(dims + (LANES,), kind)

    def held_in_hbm(value):
        return pltpu.with_memory_space_constraint(value, pltpu.HBM)

    meta = jnp.stack([labels[:, 0], wedge_index])
    away = call(
        functools.partial(split, cuts),
        (held_in_hbm(wide),),
        [HBM],
        [array((p_dev, n_z, high - low), wide.dtype) for low, high in cuts],
        scratch=[DMA((len(cuts), n_z))],
    )
    got_meta = lax.ppermute(meta, "dom", swap)
    got = [lax.ppermute(a, "dom", swap) for a in away]
    weights, begun, tally = call(
        own_sums,
        (meta, held_in_hbm(wedge_table), held_in_hbm(wide)),
        [VMEM, HBM, HBM],
        [array((n_z, wedges * stride), jnp.float32), array((n_class, n_z, rows), jnp.float32), array((n_class, SUB), jnp.float32)],
        scratch=[
            pltpu.VMEM((n_z, wedges, tiles * LANES), jnp.float32),
            pltpu.VMEM((n_z, p_dev, rows, LANES), wide.dtype),
            DMA((2, n_z)),
        ],
        flops=1 << 24,
    )

    def chip(which, by_z, shapes):
        low, high = cuts[which]
        return call(
            functools.partial(chip_sums, n_cls, n_z, by_z, low, stride),
            (got_meta, got[which], weights, begun, tally),
            [VMEM] * 5,
            shapes,
            scratch=[
                pltpu.VMEM((n_class, high - low, LANES), jnp.float32),
                pltpu.VMEM((n_class, SUB, LANES), jnp.float32),
            ],
        )

    def over(axis, moves, arrays):
        moved = list(arrays)
        for i in range(1, len(moves)):
            moved[i] = lax.ppermute(arrays[i], axis, moves[i])
        return moved

    def fold(body, count, arrays, shapes):
        return call(
            functools.partial(body, n_cls, n_z),
            tuple(arrays),
            [VMEM] * count,
            shapes,
        )

    size = [high - low for low, high in cuts]
    head = over("cls", cls_moves, chip(0, False, [array((CLS_GROUP, n_z, size[0]), jnp.int16)] * n_cls))
    ends = chip(1, True, [array((n_class, size[1]), jnp.int16)] * n_z)
    ends = over("dom", z_moves, ends)
    head = fold(sum_cls, n_cls, head, [array((CLS_GROUP, size[0]), jnp.int16)] * n_z)
    head = over("dom", z_moves, head)
    ends = fold(sum_z, n_z, ends, [array((CLS_GROUP, size[1]), jnp.int16)] * n_cls)
    ends = over("cls", cls_moves, ends)
    average, totals = call(
        functools.partial(finish, n_cls, n_z, cuts, wedges),
        (weights, *head, *ends),
        [VMEM] * (1 + n_z + n_cls),
        [array((CLS_GROUP, rows), jnp.float32), array((tiles * CLS_GROUP,), jnp.float32)],
        scratch=[pltpu.VMEM((CLS_GROUP, rows, LANES), jnp.float32)],
    )
    average = average.reshape(CLS_GROUP, tiles, parts, LANES).transpose(0, 2, 1, 3)
    average = with_layout_constraint(average, Layout(major_to_minor=(0, 2, 1, 3)))
    totals = totals.reshape(tiles, CLS_GROUP, LANES).transpose(1, 0, 2)
    totals = with_layout_constraint(totals, Layout(major_to_minor=(1, 0, 2)))
    return average.reshape(CLS_GROUP, parts, -1), totals.reshape(CLS_GROUP, -1)


def solution(mesh):
    return jax.shard_map(
        per_device,
        mesh=mesh,
        in_specs=(P(("cls", "dom"), None, None), P(("cls", "dom"), None), P(("cls", "dom")), P()),
        out_specs=(P("cls", None, "dom"), P("cls", "dom")),
        check_vma=False,
    )
```

```python
import functools

import jax
import jax.numpy as jnp
from jax import lax
from jax.experimental import pallas as pl
from jax.experimental.layout import Layout, with_layout_constraint
from jax.experimental.pallas import tpu as pltpu
from jax.sharding import PartitionSpec as P


CLS_GROUP = 2
LANES = 128
SUB = 8
CORES = 2
PARTS = 2
STEPS = 8
CUT = 63
TOP = 32000.0
LEAST = 1e-30
VMEM = pl.BlockSpec(memory_space=pltpu.VMEM)
HBM = pl.BlockSpec(memory_space=pltpu.HBM)
DMA = pltpu.SemaphoreType.DMA


def up(rows, step=SUB):
    return -(-rows // step) * step


def position():
    dom = lax.axis_index("dom")
    return lax.axis_index("cls"), lax.div(dom, CORES), lax.rem(dom, CORES)


def numbers_of(meta):
    found = meta[...]
    return [(found[0, p], found[1, p]) for p in range(meta.shape[1])]


def partner(index, offset, count):
    if count & (count - 1) == 0:
        return index ^ offset
    return (index + offset) % count


def tiles_of(first, rows):
    return (up(rows) - SUB, SUB - 2) if first else (0, 0)


def pack(total, counts, first):
    rows = total.shape[0]
    base, place = tiles_of(first, rows)
    row = lax.broadcasted_iota(jnp.int32, (SUB, LANES), 0)
    edge = total[base : base + SUB]
    edge = jnp.where(row < SUB - 2 if first else row >= SUB - 2, edge, 0.0)
    pieces = [total[:base], edge] if first else [edge, total[SUB:]]
    peak = jnp.full((1, LANES), LEAST, jnp.float32)
    for piece in pieces:
        peak = jnp.maximum(peak, jnp.max(jnp.abs(piece), axis=0, keepdims=True))
    level = jnp.ceil(jnp.log2(peak) * STEPS)
    inverse = TOP * jnp.exp2(level * (-1.0 / STEPS))
    coded = [jnp.round(piece * inverse) for piece in pieces]
    at = 1 if first else 0
    coded[at] = jnp.where(row == place, level, jnp.where(row == place + 1, counts, coded[at]))
    return jnp.concatenate(coded, axis=0).astype(jnp.int32).astype(jnp.int16)


def unpack(coded, first):
    base, place = tiles_of(first, coded.shape[0])
    wide = coded.astype(jnp.int32).astype(jnp.float32)
    at = base + place
    scale = jnp.exp2(wide[at : at + 1] * (1.0 / STEPS)) * (1.0 / TOP)
    return wide * scale, wide[at + 1 : at + 2]


def join(parts, index, first):
    value, counts = unpack(parts[0][index], first)
    for part in parts[1:]:
        more, extra = unpack(part[index], first)
        value, counts = value + more, counts + extra
    return value, counts


def split(cuts, wide, *rest):
    pos = position()
    outs, sems = rest[: len(cuts)], rest[-1]
    n_z = outs[0].shape[1]
    copies = []
    for i, (low, high) in enumerate(cuts):
        for z in range(n_z):
            source = wide.at[:, z * CORES + 1 - pos[2], low:high]
            copies.append(pltpu.make_async_copy(source, outs[i].at[:, z], sems.at[i, z]))
    for copy in copies:
        copy.start()
    for copy in copies:
        copy.wait()


def own_sums(meta, table, wide, weights, total, tally, table_buf, wide_buf, sems):
    pos = position()
    n_z, _, rows = wide_buf.shape[:3]
    wedges, length = table_buf.shape[1:]
    stride = weights.shape[1] // wedges
    copies = []
    for z in range(n_z):
        shard = z * CORES + pos[2]
        source = table.at[:, pl.ds(pl.multiple_of(shard * length, LANES), length)]
        first = pltpu.make_async_copy(source, table_buf.at[z], sems.at[0, z])
        second = pltpu.make_async_copy(wide.at[:, shard], wide_buf.at[z], sems.at[1, z])
        first.start()
        second.start()
        copies.append((first, second))
    named = numbers_of(meta)
    for z in range(n_z):
        for k in range(total.shape[0]):
            total[k, z] = jnp.zeros_like(total[k, z])
    tally[...] = jnp.zeros_like(tally)
    lane = lax.broadcasted_iota(jnp.int32, (SUB, LANES), 1)
    for k, w in named:
        tally[k] += jnp.where(lane == w, 1.0, 0.0)
    for z in range(n_z):
        copies[z][0].wait()
        for t in range(rows // PARTS):
            for base in range(0, wedges, SUB):
                count = min(SUB, wedges - base)
                tile = table_buf[z, base : base + count, t * LANES : (t + 1) * LANES]
                for c in range(PARTS):
                    weights[z, pl.ds(base * stride + t * PARTS + c, count, stride=stride), :] = tile
        copies[z][1].wait()

        for p, (k, w) in enumerate(named):
            start = pl.multiple_of(w * stride, SUB)
            total[k, z] += weights[z, pl.ds(start, rows), :] * wide_buf[z, p].astype(jnp.float32)


def chip_sums(n_cls, n_z, by_z, low, stride, got_meta, got, weights, begun, own_tally, *rest):
    pos = position()
    outs, total, tally = rest[:-2], rest[-2], rest[-1]
    classes, rows = total.shape[0], total.shape[1]
    held = classes // n_cls
    named = numbers_of(got_meta)
    lane = lax.broadcasted_iota(jnp.int32, (SUB, LANES), 1)
    tally[...] = own_tally[...]
    for k, w in named:
        tally[k] += jnp.where(lane == w, 1.0, 0.0)
    for j in range(n_z):
        zz = partner(pos[1], j, n_z)
        for k in range(classes):
            total[k] = begun[k, zz, low : low + rows]
        for p, (k, w) in enumerate(named):
            start = pl.multiple_of(w * stride + low, SUB)
            total[k] += weights[zz, pl.ds(start, rows), :] * got[p, zz].astype(jnp.float32)
        if by_z:
            for k in range(classes):
                outs[j][k] = pack(total[k], tally[k, 0:1], False)
        else:
            for i in range(n_cls):
                to = partner(pos[0], i, n_cls)
                for h in range(held):
                    k = to * held + h
                    outs[i][h, zz] = pack(total[k], tally[k, 0:1], True)


def sum_cls(n_cls, n_z, *refs):
    pos = position()
    parts, outs = refs[:n_cls], refs[n_cls:]
    for j in range(n_z):
        zz = partner(pos[1], j, n_z)
        for h in range(parts[0].shape[0]):
            outs[j][h] = pack(*join(parts, (h, zz), True), True)


def sum_z(n_cls, n_z, *refs):
    pos = position()
    parts, outs = refs[:n_z], refs[n_z:]
    held = parts[0].shape[0] // n_cls
    for i in range(n_cls):
        to = partner(pos[0], i, n_cls)
        for h in range(held):
            outs[i][h] = pack(*join(parts, (to * held + h,), False), False)


def finish(n_cls, n_z, cuts, wedges, weights, *refs):
    pos = position()
    sides = (refs[:n_z], refs[n_z : n_z + n_cls])
    out, out_totals, scratch, average, totals, sems = refs[n_z + n_cls :]
    stride = weights.shape[1] // wedges
    held, rows = average.shape[0], average.shape[1]
    shape = (up(wedges), LANES)
    lane, place = lax.broadcasted_iota(jnp.int32, shape, 1), lax.broadcasted_iota(jnp.int32, shape, 0)
    heads = [join(sides[0], (h,), True) for h in range(held)]
    ends = [join(sides[1], (h,), False)[0] for h in range(held)]
    numbers = [
        jnp.sum(jnp.where(lane == place, counts, 0.0), axis=1, keepdims=True) for _, counts in heads
    ]
    cut = cuts[1][0]
    row = lax.broadcasted_iota(jnp.int32, (SUB, LANES), 0)
    pieces = ((0, cut), (cut, cut + SUB), (cut + SUB, rows))
    for low, high in pieces:
        weight = [jnp.zeros((high - low, LANES), jnp.float32) for _ in range(held)]
        for w in range(wedges):
            one = weights[pos[1], w * stride + low : w * stride + high]
            square = one * one
            for h in range(held):
                weight[h] = weight[h] + numbers[h][w : w + 1] * square
        for h in range(held):
            if low == 0:
                sums = heads[h][0][:cut]
            elif low == cut:
                sums = jnp.where(row < SUB - 2, heads[h][0][cut:], ends[h][:SUB])
            else:
                sums = ends[h][SUB:]
            scratch[h, low:high] = weight[h]
            average[h, low:high] = sums / (weight[h] + 1.0)
        if low == 0:
            first = pltpu.make_async_copy(average.at[:, :cut], out.at[:, :cut], sems.at[0])
            first.start()
    for h in range(held):
        tiles = rows // PARTS
        totals[pl.ds(h, tiles, stride=held), :] = scratch[h, pl.ds(0, tiles, stride=PARTS), :]
    second = pltpu.make_async_copy(average.at[:, cut:rows], out.at[:, cut:rows], sems.at[1])
    third = pltpu.make_async_copy(totals, out_totals, sems.at[2])
    second.start()
    third.start()
    for copy in (first, second, third):
        copy.wait()


def call(body, operands, specs, shapes, scratch=(), flops=1 << 22, limit=16, places=None):
    return pl.pallas_call(
        body,
        out_shape=shapes,
        in_specs=specs,
        out_specs=places or [VMEM] * len(shapes),
        scratch_shapes=list(scratch),
        compiler_params=pltpu.CompilerParams(vmem_limit_bytes=limit * 1024 * 1024),
        cost_estimate=pl.CostEstimate(flops=flops, bytes_accessed=flops, transcendentals=0),
    )(*operands)


def per_device(particles, labels, wedge_index, wedge_table):
    n_cls, n_dom = lax.axis_size("cls"), lax.axis_size("dom")
    n_z = n_dom // CORES
    n_class = n_cls * CLS_GROUP
    p_dev, parts, voxels = particles.shape
    wedges = wedge_table.shape[0]
    tiles = voxels // (n_dom * LANES)
    rows = tiles * parts
    stride = up(rows)

    swap = [(d, d ^ 1) for d in range(n_dom)]
    z_moves = [
        [(d, partner(d // CORES, j, n_z) * CORES + d % CORES) for d in range(n_dom)] for j in range(n_z)
    ]
    cls_moves = [[(d, partner(d, i, n_cls)) for d in range(n_cls)] for i in range(n_cls)]

    cut = rows * CUT // 100 // SUB * SUB
    cuts = ((0, cut + SUB), (cut, rows))
    wide = particles.reshape(p_dev, parts, n_dom * tiles, LANES).transpose(0, 2, 1, 3)
    wide = wide.reshape(p_dev, n_dom, rows, LANES)

    def array(dims, kind):
        return jax.ShapeDtypeStruct(dims + (LANES,), kind)

    def held_in_hbm(value):
        return pltpu.with_memory_space_constraint(value, pltpu.HBM)

    meta = jnp.stack([labels[:, 0], wedge_index])
    away = call(
        functools.partial(split, cuts),
        (held_in_hbm(wide),),
        [HBM],
        [array((p_dev, n_z, high - low), wide.dtype) for low, high in cuts],
        scratch=[DMA((len(cuts), n_z))],
    )
    got_meta = lax.ppermute(meta, "dom", swap)
    got = [lax.ppermute(a, "dom", swap) for a in away]
    weights, begun, tally = call(
        own_sums,
        (meta, held_in_hbm(wedge_table), held_in_hbm(wide)),
        [VMEM, HBM, HBM],
        [array((n_z, wedges * stride), jnp.float32), array((n_class, n_z, rows), jnp.float32), array((n_class, SUB), jnp.float32)],
        scratch=[
            pltpu.VMEM((n_z, wedges, tiles * LANES), jnp.float32),
            pltpu.VMEM((n_z, p_dev, rows, LANES), wide.dtype),
            DMA((2, n_z)),
        ],
        flops=1 << 24,
    )

    def chip(which, by_z, shapes):
        low, high = cuts[which]
        return call(
            functools.partial(chip_sums, n_cls, n_z, by_z, low, stride),
            (got_meta, got[which], weights, begun, tally),
            [VMEM] * 5,
            shapes,
            scratch=[
                pltpu.VMEM((n_class, high - low, LANES), jnp.float32),
                pltpu.VMEM((n_class, SUB, LANES), jnp.float32),
            ],
        )

    def over(axis, moves, arrays):
        moved = list(arrays)
        for i in range(1, len(moves)):
            moved[i] = lax.ppermute(arrays[i], axis, moves[i])
        return moved

    def fold(body, count, arrays, shapes):
        return call(
            functools.partial(body, n_cls, n_z),
            tuple(arrays),
            [VMEM] * count,
            shapes,
        )

    size = [high - low for low, high in cuts]
    head = over("cls", cls_moves, chip(0, False, [array((CLS_GROUP, n_z, size[0]), jnp.int16)] * n_cls))
    ends = chip(1, True, [array((n_class, size[1]), jnp.int16)] * n_z)
    ends = over("dom", z_moves, ends)
    head = fold(sum_cls, n_cls, head, [array((CLS_GROUP, size[0]), jnp.int16)] * n_z)
    head = over("dom", z_moves, head)
    ends = fold(sum_z, n_z, ends, [array((CLS_GROUP, size[1]), jnp.int16)] * n_cls)
    ends = over("cls", cls_moves, ends)
    average, totals = call(
        functools.partial(finish, n_cls, n_z, cuts, wedges),
        (weights, *head, *ends),
        [VMEM] * (1 + n_z + n_cls),
        [array((CLS_GROUP, rows), jnp.float32), array((tiles * CLS_GROUP,), jnp.float32)],
        scratch=[
            pltpu.VMEM((CLS_GROUP, rows, LANES), jnp.float32),
            pltpu.VMEM((CLS_GROUP, rows, LANES), jnp.float32),
            pltpu.VMEM((tiles * CLS_GROUP, LANES), jnp.float32),
            DMA((3,)),
        ],
        places=[HBM, HBM],
    )
    average = average.reshape(CLS_GROUP, tiles, parts, LANES).transpose(0, 2, 1, 3)
    average = with_layout_constraint(average, Layout(major_to_minor=(0, 2, 1, 3)))
    totals = totals.reshape(tiles, CLS_GROUP, LANES).transpose(1, 0, 2)
    totals = with_layout_constraint(totals, Layout(major_to_minor=(1, 0, 2)))
    return average.reshape(CLS_GROUP, parts, -1), totals.reshape(CLS_GROUP, -1)


def solution(mesh):
    return jax.shard_map(
        per_device,
        mesh=mesh,
        in_specs=(P(("cls", "dom"), None, None), P(("cls", "dom"), None), P(("cls", "dom")), P()),
        out_specs=(P("cls", None, "dom"), P("cls", "dom")),
        check_vma=False,
    )
```
